32 devices in a mesh: dp: 1 (over z), ep: 32 (over y, x, core).
Axes of the slice: x: 4, y: 4, z: 1, core: 2. Of those that a mesh axis runs over, the one named last changes fastest.
The devices are a block of a 4x4x8 slice.
Arguments:
- x_rows: bfloat16 [131072, 1024], P(('dp', 'ep'))
- sel_idx: int32 [32, 8192], P(('dp', 'ep'))
- gate_w: float32 [32, 8192], P(('dp', 'ep'))
- w_up: bfloat16 [32, 1024, 2816], P('ep')
- w_down: bfloat16 [32, 2816, 1024], P('ep')
Outputs:
- output: bfloat16 [131072, 1024], P(('dp', 'ep'))
All inputs are finite; a program needn't handle non-finite values.
Results may differ from the reference program's by a relative error of at most 0.00679449.
Values are sent between devices in bfloat16 or wider.
A program may use at most 768 MiB of HBM per device.

```python
import jax
import jax.numpy as jnp
from jax import lax

D_MODEL = 1024
D_FF = 2816
EXPERTS = 32
GROUP_SIZE = 32
TOKENS = 131072
CAPACITY = 8192

TOK_LOC = TOKENS // GROUP_SIZE
EXP_LOC = EXPERTS // GROUP_SIZE
PER_SOURCE = CAPACITY // GROUP_SIZE


def draw_selection(sel_key):
    key_order, key_hot, key_rank, key_delta, key_rows, key_cols = jax.random.split(sel_key, 6)
    dev_order = jax.random.permutation(key_order, GROUP_SIZE)
    hot_owner = dev_order[jax.random.randint(key_hot, (GROUP_SIZE,), 0, max(1, GROUP_SIZE // 4))]
    hot_expert = jnp.repeat(hot_owner, EXP_LOC)
    rank_keys = jax.random.randint(key_rank, (EXPERTS, GROUP_SIZE), 0, 1048576)
    rank_keys = jnp.where(jnp.arange(GROUP_SIZE)[None, :] == hot_expert[:, None], -1, rank_keys)
    src_order = jnp.argsort(rank_keys, axis=1, stable=True)
    delta_rows = jax.random.randint(key_delta, (EXPERTS, (GROUP_SIZE - 2) // 2), 0, PER_SOURCE + 1)
    paired = jnp.stack([PER_SOURCE + delta_rows, PER_SOURCE - delta_rows], axis=2).reshape(EXPERTS, GROUP_SIZE - 2)
    count_by_pos = jnp.concatenate([jnp.full((EXPERTS, 1), 2 * PER_SOURCE, jnp.int32), paired.astype(jnp.int32), jnp.zeros((EXPERTS, 1), jnp.int32)], axis=1)
    count_dev = jnp.take_along_axis(count_by_pos, jnp.argsort(src_order, axis=1), axis=1)
    row_ends = jnp.cumsum(count_dev, axis=1)
    row_starts = row_ends - count_dev
    slot_ids = jnp.arange(CAPACITY)
    source = jnp.sum((row_ends[:, None, :] <= slot_ids[None, :, None]).astype(jnp.int32), axis=2)
    rank_in = slot_ids[None, :] - jnp.take_along_axis(row_starts, source, axis=1)
    row_perm = jnp.argsort(jax.random.bits(key_rows, (EXPERTS, GROUP_SIZE, TOK_LOC)), axis=2).reshape(EXPERTS, TOKENS)
    picked = jnp.take_along_axis(row_perm, source * TOK_LOC + rank_in, axis=1)
    tokens = source * TOK_LOC + picked
    col_perm = jnp.argsort(jax.random.bits(key_cols, (EXPERTS, CAPACITY)), axis=1)
    return jnp.take_along_axis(tokens, col_perm, axis=1).astype(jnp.int32)


def setup_inputs(seed: int = 0, part: int = 0) -> dict:
    base_key = jax.random.key(seed)
    part_key = jax.random.fold_in(base_key, part)
    key_x, key_sel, key_gate = jax.random.split(part_key, 3)
    key_up, key_down = jax.random.split(jax.random.key(seed + 1), 2)
    up_scale = D_MODEL ** -0.5
    down_scale = 1.5 * D_FF ** -0.5
    x_rows = jax.random.normal(key_x, (TOKENS, D_MODEL), jnp.float32).astype(jnp.bfloat16)
    sel_idx = draw_selection(key_sel)
    gate_w = jax.random.uniform(key_gate, (EXPERTS, CAPACITY), jnp.float32, 0.25, 1.25)
    w_up = (jax.random.normal(key_up, (EXPERTS, D_MODEL, D_FF), jnp.float32) * up_scale).astype(jnp.bfloat16)
    w_down = (jax.random.normal(key_down, (EXPERTS, D_FF, D_MODEL), jnp.float32) * down_scale).astype(jnp.bfloat16)
    return {"x_rows": x_rows, "sel_idx": sel_idx, "gate_w": gate_w, "w_up": w_up, "w_down": w_down}


def reference(x_rows, sel_idx, gate_w, w_up, w_down):
    def one_expert(expert_args):
        sel_row, gate_row, up_mat, down_mat = expert_args
        chosen = jnp.take(x_rows, sel_row, axis=0)
        hidden = jax.nn.gelu(jnp.dot(chosen, up_mat, preferred_element_type=jnp.float32), approximate=True).astype(jnp.bfloat16)
        out_rows = jnp.dot(hidden, down_mat, preferred_element_type=jnp.float32)
        return (out_rows * gate_row[:, None]).astype(jnp.bfloat16)

    contrib = lax.map(one_expert, (sel_idx, gate_w, w_up, w_down))
    summed = jax.ops.segment_sum(contrib.reshape(EXPERTS * CAPACITY, D_MODEL).astype(jnp.float32), sel_idx.reshape(EXPERTS * CAPACITY), num_segments=TOKENS)
    return (x_rows.astype(jnp.float32) + summed).astype(jnp.bfloat16)
```

```python
import jax
import jax.numpy as jnp
from jax import lax
from jax.sharding import PartitionSpec as P

CHUNKS = 4


def solution(mesh):
    group_size = mesh.shape["ep"]

    def local_layer(x_loc, sel_loc, gate_loc, up_loc, down_loc):
        tok_loc, model_width = x_loc.shape
        entry_count = sel_loc.shape[0] * sel_loc.shape[1]
        pair_cap = 2 * entry_count // group_size
        part = pair_cap // CHUNKS
        sel = sel_loc.reshape(entry_count)
        dev_ids = jnp.arange(group_size, dtype=jnp.int32)
        src_dev = sel // tok_loc
        counts = jnp.sum((src_dev[:, None] == dev_ids[None, :]).astype(jnp.int32), axis=0)
        lower = dev_ids[:, None] >= dev_ids[None, :]
        free_end = jnp.sum(jnp.where(lower, (pair_cap - counts)[None, :], 0), axis=1)
        fill_ids = jnp.arange(group_size * pair_cap - entry_count, dtype=jnp.int32)
        fill_dev = jnp.sum((free_end[None, :] <= fill_ids[:, None]).astype(jnp.int32), axis=1)
        keys = jnp.concatenate([sel + src_dev * tok_loc, fill_dev * (2 * tok_loc) + tok_loc])
        gates = jnp.concatenate([gate_loc.reshape(entry_count), jnp.zeros(fill_ids.shape, jnp.float32)])
        keys, gates = lax.sort((keys, gates), num_keys=1, is_stable=False)
        request = keys.reshape(group_size, pair_cap) - dev_ids[:, None] * (2 * tok_loc)
        gates = gates.reshape(group_size, pair_cap)
        wanted = lax.all_to_all(request, "ep", 0, 0, tiled=True)

        rows = group_size * part
        acc = x_loc.astype(jnp.float32)
        sent = []
        for k in range(CHUNKS):
            idx = wanted[:, k * part:(k + 1) * part].reshape(rows)
            send = x_loc.at[jnp.minimum(idx, tok_loc - 1)].get(mode="promise_in_bounds")
            sent.append((idx, lax.all_to_all(send.reshape(group_size, part, model_width), "ep", 0, 0, tiled=True)))
        back = []
        for k in range(CHUNKS):
            idx, got = sent[k]
            hidden = jax.nn.gelu(jnp.dot(got.reshape(rows, model_width), up_loc[0], preferred_element_type=jnp.float32), approximate=True).astype(jnp.bfloat16)
            out = jnp.dot(hidden, down_loc[0], preferred_element_type=jnp.float32)
            gate = gates[:, k * part:(k + 1) * part].reshape(rows, 1)
            contrib = (out * gate).astype(jnp.bfloat16).reshape(group_size, part, model_width)
            back.append((idx, lax.all_to_all(contrib, "ep", 0, 0, tiled=True)))
        for idx, ret in back:
            acc = acc.at[idx].add(ret.reshape(rows, model_width).astype(jnp.float32), mode="drop")
        return acc.astype(jnp.bfloat16)

    row_spec = P(("dp", "ep"), None)
    weight_spec = P("ep", None, None)
    return jax.shard_map(local_layer, mesh=mesh, in_specs=(row_spec, row_spec, row_spec, weight_spec, weight_spec), out_specs=row_spec, check_vma=False)
```

```python
import functools

import jax
import jax.numpy as jnp
from jax import lax
from jax.experimental import pallas as pl
from jax.experimental.pallas import tpu as pltpu
from jax.sharding import PartitionSpec as P

CHUNKS = 2
LANES = 128
BATCH = 8
VMEM_LIMIT = 60 * 1024 * 1024


def pack_kernel(idx_ref, x_ref, out_ref):
    rows = out_ref.shape[0]
    base = pl.program_id(0) * rows

    def body(b, _):
        vals = [x_ref[idx_ref[base + b * BATCH + j]] for j in range(BATCH)]
        for j in range(BATCH):
            out_ref[b * BATCH + j] = vals[j]
        return 0

    lax.fori_loop(0, rows // BATCH, body, 0)


def pack_rows(x3, idx, block):
    rows = idx.shape[0]
    tail = x3.shape[1:]
    return pl.pallas_call(
        pack_kernel,
        grid_spec=pltpu.PrefetchScalarGridSpec(
            num_scalar_prefetch=1,
            grid=(rows // block,),
            in_specs=[pl.BlockSpec(x3.shape, lambda i, idx: (0, 0, 0))],
            out_specs=pl.BlockSpec((block,) + tail, lambda i, idx: (i, 0, 0)),
        ),
        out_shape=jax.ShapeDtypeStruct((rows,) + tail, x3.dtype),
        compiler_params=pltpu.CompilerParams(vmem_limit_bytes=VMEM_LIMIT),
        cost_estimate=pl.CostEstimate(flops=rows * 4096, bytes_accessed=rows * 4096, transcendentals=0),
    )(idx, x3)


def combine_kernel(idx_ref, cnt_ref, base_ref, ret_ref, out_ref, acc, sem):
    g = pl.program_id(0)
    part = ret_ref.shape[0]
    tok = base_ref.shape[0]

    @pl.when(g == 0)
    def _():
        load = pltpu.make_async_copy(base_ref, acc.at[pl.ds(0, tok)], sem)
        load.start()
        load.wait()

    def body(b, _):
        at = [idx_ref[g * part + b * BATCH + j] for j in range(BATCH)]
        sums = [acc[at[j]] + ret_ref[b * BATCH + j].astype(jnp.float32) for j in range(BATCH)]
        for j in range(BATCH):
            acc[at[j]] = sums[j]
        return 0

    lax.fori_loop(0, (cnt_ref[g] + BATCH - 1) // BATCH, body, 0)

    @pl.when(g == pl.num_programs(0) - 1)
    def _():
        store = pltpu.make_async_copy(acc.at[pl.ds(0, tok)], out_ref, sem)
        store.start()
        store.wait()


def combine_rows(base, ret, idx, cnt):
    group, part = ret.shape[:2]
    tail = base.shape[1:]
    return pl.pallas_call(
        combine_kernel,
        grid_spec=pltpu.PrefetchScalarGridSpec(
            num_scalar_prefetch=2,
            grid=(group,),
            in_specs=[
                pl.BlockSpec(memory_space=pl.ANY),
                pl.BlockSpec((None, part) + tail, lambda g, idx, cnt: (g, 0, 0, 0)),
            ],
            out_specs=pl.BlockSpec(memory_space=pl.ANY),
            scratch_shapes=[pltpu.VMEM((base.shape[0] + 8,) + tail, jnp.float32), pltpu.SemaphoreType.DMA],
        ),
        out_shape=jax.ShapeDtypeStruct(base.shape, jnp.float32),
        compiler_params=pltpu.CompilerParams(vmem_limit_bytes=VMEM_LIMIT),
        cost_estimate=pl.CostEstimate(flops=group * part * 4096, bytes_accessed=group * part * 6144, transcendentals=0),
    )(idx, cnt, base, ret)


def solution(mesh):
    group_size = mesh.shape["ep"]

    def local_layer(x_loc, sel_loc, gate_loc, up_loc, down_loc):
        tok_loc, model_width = x_loc.shape
        tail = (model_width // LANES, LANES)
        entry_count = sel_loc.shape[0] * sel_loc.shape[1]
        pair_cap = 2 * entry_count // group_size
        part = pair_cap // CHUNKS
        sel = sel_loc.reshape(entry_count)
        dev_ids = jnp.arange(group_size, dtype=jnp.int32)
        src_dev = sel // tok_loc
        counts = jnp.sum((src_dev[:, None] == dev_ids[None, :]).astype(jnp.int32), axis=0)
        lower = dev_ids[:, None] >= dev_ids[None, :]
        free_end = jnp.sum(jnp.where(lower, (pair_cap - counts)[None, :], 0), axis=1)
        fill_ids = jnp.arange(group_size * pair_cap - entry_count, dtype=jnp.int32)
        fill_dev = jnp.sum((free_end[None, :] <= fill_ids[:, None]).astype(jnp.int32), axis=1)
        keys = jnp.concatenate([sel + src_dev * tok_loc, fill_dev * (2 * tok_loc) + tok_loc])
        gates = jnp.concatenate([gate_loc.reshape(entry_count), jnp.zeros(fill_ids.shape, jnp.float32)])
        keys, gates = lax.sort((keys, gates), num_keys=1, is_stable=False)
        request = keys.reshape(group_size, pair_cap) - dev_ids[:, None] * (2 * tok_loc)
        gates = gates.reshape(group_size, pair_cap)
        wanted = lax.all_to_all(request, "ep", 0, 0, tiled=True)
        filled = jnp.sum((wanted < tok_loc).astype(jnp.int32), axis=1)

        rows = group_size * part
        x3 = x_loc.reshape((tok_loc,) + tail)
        sent = []
        for k in range(CHUNKS):
            idx = wanted[:, k * part:(k + 1) * part].reshape(rows)
            send = pack_rows(x3, jnp.minimum(idx, tok_loc - 1), rows // 8)
            sent.append((idx, lax.all_to_all(send.reshape((group_size, part) + tail), "ep", 0, 0, tiled=True)))
        back = []
        for k in range(CHUNKS):
            idx, got = sent[k]
            hidden = jax.nn.gelu(jnp.dot(got.reshape(rows, model_width), up_loc[0], preferred_element_type=jnp.float32), approximate=True).astype(jnp.bfloat16)
            out = jnp.dot(hidden, down_loc[0], preferred_element_type=jnp.float32)
            gate = gates[:, k * part:(k + 1) * part].reshape(rows, 1)
            contrib = (out * gate).astype(jnp.bfloat16).reshape((group_size, part) + tail)
            back.append((idx, lax.all_to_all(contrib, "ep", 0, 0, tiled=True)))
        acc = x3.astype(jnp.float32)
        for k, (idx, ret) in enumerate(back):
            acc = combine_rows(acc, ret, idx, jnp.clip(filled - k * part, 0, part))
        return acc.reshape(tok_loc, model_width).astype(jnp.bfloat16)

    row_spec = P(("dp", "ep"), None)
    weight_spec = P("ep", None, None)
    return jax.shard_map(local_layer, mesh=mesh, in_specs=(row_spec, row_spec, row_spec, weight_spec, weight_spec), out_specs=row_spec, check_vma=False)
```

```python
import functools
import math

import jax
import jax.numpy as jnp
from jax import lax
from jax.experimental import pallas as pl
from jax.experimental.pallas import tpu as pltpu
from jax.sharding import PartitionSpec as P

LANES = 128
BATCH = 8
VMEM_LIMIT = 60 * 1024 * 1024
SEND_SLOTS = 8
OUT_SLOTS = 6
AHEAD = 6
STRIDE = 13
COLS = 256
STEP = 128


def peers(k, group, side):
    me = lax.axis_index("ep")
    d = (k * STRIDE) % group
    dy, dx, dc = d // (2 * side), (d // 2) % side, d % 2
    y, x, c = me // (2 * side), (me // 2) % side, me % 2
    to = (((y + dy) % side) * side + (x + dx) % side) * 2 + (c + dc) % 2
    frm = (((y + side - dy) % side) * side + (x + side - dx) % side) * 2 + (c + 2 - dc) % 2
    return to, frm


def moe_kernel(group, side, idx_ref, x_ref, up_ref, down_ref, gate_ref, recv_ref, ret_ref,
               rows, send, blk, gblk, hid, out, send_sem, out_sem, recv_sem, ret_sem, load_sem):
    me = lax.axis_index("ep")
    cap, sub = rows.shape[0], rows.shape[1]

    barrier = pltpu.get_barrier_semaphore()

    def hello(d, _):
        pl.semaphore_signal(barrier, inc=1, device_id={"ep": (me + d) % group}, device_id_type=pl.DeviceIdType.MESH)
        return 0

    lax.fori_loop(1, group, hello, 0)
    pl.semaphore_wait(barrier, group - 1)

    def dispatch(k):
        to, _ = peers(k, group, side)
        return pltpu.make_async_remote_copy(
            src_ref=send.at[k % SEND_SLOTS], dst_ref=recv_ref.at[me], send_sem=send_sem.at[k % SEND_SLOTS],
            recv_sem=recv_sem.at[k], device_id={"ep": to}, device_id_type=pl.DeviceIdType.MESH)

    def give_back(k):
        _, frm = peers(k, group, side)
        return pltpu.make_async_remote_copy(
            src_ref=out.at[k % OUT_SLOTS], dst_ref=ret_ref.at[me], send_sem=out_sem.at[k % OUT_SLOTS],
            recv_sem=ret_sem.at[k], device_id={"ep": frm}, device_id_type=pl.DeviceIdType.MESH)

    def pack(to, dst):
        def pick(b, _):
            vals = [x_ref[idx_ref[to, b * BATCH + j]].astype(jnp.float32) for j in range(BATCH)]
            for j in range(BATCH):
                rows[b * BATCH + j] = vals[j]
            return 0

        lax.fori_loop(0, cap // BATCH, pick, 0)

        def flat(b, _):
            at = pl.ds(b * STEP, STEP)
            for s in range(sub):
                dst[at, s * LANES:(s + 1) * LANES] = rows[at, s, :].astype(jnp.bfloat16)
            return 0

        lax.fori_loop(0, cap // STEP, flat, 0)

    def pack_and_send(k):
        to, _ = peers(k, group, side)

        @pl.when(k > SEND_SLOTS)
        def _():
            dispatch(k - SEND_SLOTS).wait_send()

        pack(to, send.at[k % SEND_SLOTS])
        dispatch(k).start()

    def ffn_up():
        def up(f, _):
            at = pl.ds(pl.multiple_of(f * COLS, COLS), COLS)
            z = jnp.dot(blk[...], up_ref[:, at], preferred_element_type=jnp.float32)
            hid[:, at] = jax.nn.gelu(z, approximate=True).astype(jnp.bfloat16)
            return 0

        lax.fori_loop(0, up_ref.shape[1] // COLS, up, 0)

    def ffn_down(slot):
        for n in range(down_ref.shape[1] // COLS):
            o = jnp.dot(hid[...], down_ref[:, n * COLS:(n + 1) * COLS], preferred_element_type=jnp.float32)
            for t in range(COLS // LANES):
                rows[:, n * (COLS // LANES) + t, :] = o[:, t * LANES:(t + 1) * LANES] * gblk[...]

        def tile(b, _):
            at = pl.ds(b * STEP, STEP)
            out[slot, at] = rows[at].astype(jnp.bfloat16)
            return 0

        lax.fori_loop(0, cap // STEP, tile, 0)

    def own():
        load_gate = pltpu.make_async_copy(gate_ref.at[me], gblk, load_sem.at[1])
        load_gate.start()
        pack(me, blk)
        load_gate.wait()
        ffn_up()
        ffn_down(0)
        keep = pltpu.make_async_copy(out.at[0], ret_ref.at[me], load_sem.at[0])
        keep.start()
        keep.wait()

    def expert(k):
        to, frm = peers(k, group, side)
        pltpu.make_async_remote_copy(
            src_ref=send.at[0], dst_ref=recv_ref.at[frm], send_sem=send_sem.at[0], recv_sem=recv_sem.at[k],
            device_id={"ep": to}, device_id_type=pl.DeviceIdType.MESH).wait_recv()
        load_rows = pltpu.make_async_copy(recv_ref.at[frm], blk, load_sem.at[0])
        load_gate = pltpu.make_async_copy(gate_ref.at[frm], gblk, load_sem.at[1])
        load_rows.start()
        load_gate.start()
        load_rows.wait()
        load_gate.wait()
        ffn_up()

        @pl.when(k > OUT_SLOTS)
        def _():
            give_back(k - OUT_SLOTS).wait_send()

        ffn_down(k % OUT_SLOTS)
        give_back(k).start()

    def first(k, _):
        pack_and_send(k)
        return 0

    def step(k, _):
        @pl.when(k + AHEAD < group)
        def _():
            pack_and_send(k + AHEAD)

        expert(k)
        return 0

    lax.fori_loop(1, min(AHEAD + 1, group), first, 0)
    own()
    lax.fori_loop(1, group, step, 0)

    def drain_send(k, _):
        dispatch(k).wait_send()
        return 0

    def drain_out(k, _):
        give_back(k).wait_send()
        return 0

    def drain_ret(k, _):
        to, _ = peers(k, group, side)
        pltpu.make_async_remote_copy(
            src_ref=out.at[0], dst_ref=ret_ref.at[to], send_sem=out_sem.at[0], recv_sem=ret_sem.at[k],
            device_id={"ep": to}, device_id_type=pl.DeviceIdType.MESH).wait_recv()
        return 0

    lax.fori_loop(max(group - SEND_SLOTS, 1), group, drain_send, 0)
    lax.fori_loop(max(group - OUT_SLOTS, 1), group, drain_out, 0)
    lax.fori_loop(1, group, drain_ret, 0)


def moe_exchange(group, idx, x3, up, down, gates):
    side = math.isqrt(group // 2)
    assert 2 * side * side == group
    cap = idx.shape[1]
    tail = x3.shape[1:]
    width, hidden = up.shape
    any_spec = pl.BlockSpec(memory_space=pl.ANY)
    vmem_spec = pl.BlockSpec(memory_space=pltpu.VMEM)
    _, ret = pl.pallas_call(
        functools.partial(moe_kernel, group, side),
        in_specs=[pl.BlockSpec(memory_space=pltpu.SMEM), vmem_spec, vmem_spec, vmem_spec, any_spec],
        out_specs=[any_spec, any_spec],
        out_shape=[jax.ShapeDtypeStruct((group, cap, width), x3.dtype), jax.ShapeDtypeStruct((group, cap) + tail, x3.dtype)],
        scratch_shapes=[
            pltpu.VMEM((cap,) + tail, jnp.float32),
            pltpu.VMEM((SEND_SLOTS, cap, width), x3.dtype),
            pltpu.VMEM((cap, width), x3.dtype),
            pltpu.VMEM((cap, LANES), jnp.float32),
            pltpu.VMEM((cap, hidden), x3.dtype),
            pltpu.VMEM((OUT_SLOTS, cap) + tail, x3.dtype),
            pltpu.SemaphoreType.DMA((SEND_SLOTS,)),
            pltpu.SemaphoreType.DMA((OUT_SLOTS,)),
            pltpu.SemaphoreType.DMA((group,)),
            pltpu.SemaphoreType.DMA((group,)),
            pltpu.SemaphoreType.DMA((2,)),
        ],
        compiler_params=pltpu.CompilerParams(collective_id=0, has_side_effects=True, vmem_limit_bytes=VMEM_LIMIT),
        cost_estimate=pl.CostEstimate(flops=4 * group * cap * width * hidden, bytes_accessed=4 * group * cap * width, transcendentals=0),
    )(idx, x3, up, down, gates)
    return ret


def combine_kernel(idx_ref, cnt_ref, x_ref, ret_ref, out_ref, acc):
    g = pl.program_id(0)
    part = ret_ref.shape[0]
    tok, width = x_ref.shape
    sub = width // LANES

    @pl.when(g == 0)
    def _():
        def load(b, _):
            at = pl.ds(b * STEP, STEP)
            for s in range(sub):
                acc[at, s, :] = x_ref[at, s * LANES:(s + 1) * LANES].astype(jnp.float32)
            return 0

        lax.fori_loop(0, tok // STEP, load, 0)

    def body(b, _):
        at = [idx_ref[g * part + b * BATCH + j] for j in range(BATCH)]
        sums = [acc[at[j]] + ret_ref[b * BATCH + j].astype(jnp.float32) for j in range(BATCH)]
        for j in range(BATCH):
            acc[at[j]] = sums[j]
        return 0

    lax.fori_loop(0, (cnt_ref[g] + BATCH - 1) // BATCH, body, 0)

    @pl.when(g == pl.num_programs(0) - 1)
    def _():
        def store(b, _):
            at = pl.ds(b * STEP, STEP)
            for s in range(sub):
                out_ref[at, s * LANES:(s + 1) * LANES] = acc[at, s, :].astype(jnp.bfloat16)
            return 0

        lax.fori_loop(0, tok // STEP, store, 0)


def combine_rows(x_loc, ret, idx, cnt):
    group, part = ret.shape[:2]
    tail = ret.shape[2:]
    tok = x_loc.shape[0]
    whole = pl.BlockSpec(x_loc.shape, lambda g, idx, cnt: (0, 0))
    return pl.pallas_call(
        combine_kernel,
        grid_spec=pltpu.PrefetchScalarGridSpec(
            num_scalar_prefetch=2,
            grid=(group,),
            in_specs=[whole, pl.BlockSpec((None, part) + tail, lambda g, idx, cnt: (g, 0, 0, 0))],
            out_specs=whole,
            scratch_shapes=[pltpu.VMEM((tok + 8,) + tail, jnp.float32)],
        ),
        out_shape=jax.ShapeDtypeStruct(x_loc.shape, x_loc.dtype),
        compiler_params=pltpu.CompilerParams(vmem_limit_bytes=VMEM_LIMIT),
        cost_estimate=pl.CostEstimate(flops=group * part * 4096, bytes_accessed=group * part * 4096, transcendentals=0),
    )(idx, cnt, x_loc, ret)


def solution(mesh):
    group_size = mesh.shape["ep"]

    def local_layer(x_loc, sel_loc, gate_loc, up_loc, down_loc):
        tok_loc, model_width = x_loc.shape
        tail = (model_width // LANES, LANES)
        entry_count = sel_loc.shape[0] * sel_loc.shape[1]
        pair_cap = 2 * entry_count // group_size
        sel = sel_loc.reshape(entry_count)
        dev_ids = jnp.arange(group_size, dtype=jnp.int32)
        src_dev = sel // tok_loc
        counts = jnp.sum((src_dev[:, None] == dev_ids[None, :]).astype(jnp.int32), axis=0)
        lower = dev_ids[:, None] >= dev_ids[None, :]
        free_end = jnp.sum(jnp.where(lower, (pair_cap - counts)[None, :], 0), axis=1)
        fill_ids = jnp.arange(group_size * pair_cap - entry_count, dtype=jnp.int32)
        fill_dev = jnp.sum((free_end[None, :] <= fill_ids[:, None]).astype(jnp.int32), axis=1)
        keys = jnp.concatenate([sel + src_dev * tok_loc, fill_dev * (2 * tok_loc) + tok_loc])
        gates = jnp.concatenate([gate_loc.reshape(entry_count), jnp.zeros(fill_ids.shape, jnp.float32)])
        keys, gates = lax.sort((keys, gates), num_keys=1, is_stable=False)
        request = keys.reshape(group_size, pair_cap) - dev_ids[:, None] * (2 * tok_loc)
        gates = jnp.broadcast_to(gates.reshape(group_size, pair_cap)[:, :, None], (group_size, pair_cap, LANES))
        wanted = lax.all_to_all(request, "ep", 0, 0, tiled=True)
        filled = jnp.sum((wanted < tok_loc).astype(jnp.int32), axis=1)
        x3 = x_loc.reshape((tok_loc,) + tail)
        ret = moe_exchange(group_size, jnp.minimum(wanted, tok_loc - 1), x3, up_loc[0], down_loc[0], gates)
        return combine_rows(x_loc, ret, wanted.reshape(group_size * pair_cap), filled)

    row_spec = P(("dp", "ep"), None)
    weight_spec = P("ep", None, None)
    return jax.shard_map(local_layer, mesh=mesh, in_specs=(row_spec, row_spec, row_spec, weight_spec, weight_spec), out_specs=row_spec, check_vma=False)
```

```python
import functools
import math

import jax
import jax.numpy as jnp
from jax import lax
from jax.experimental import pallas as pl
from jax.experimental.pallas import tpu as pltpu
from jax.sharding import PartitionSpec as P

LANES = 128
BATCH = 8
ADD_BATCH = 16
VMEM_LIMIT = 60 * 1024 * 1024
SEND_SLOTS = 14
OUT_SLOTS = 10
AHEAD = 13
STRIDE = 13
COLS = 256
STEP = 128


def peers(k, group, side):
    me = lax.axis_index("ep")
    d = (k * STRIDE) % group
    dy, dx, dc = d // (2 * side), (d // 2) % side, d % 2
    y, x, c = me // (2 * side), (me // 2) % side, me % 2
    to = (((y + dy) % side) * side + (x + dx) % side) * 2 + (c + dc) % 2
    frm = (((y + side - dy) % side) * side + (x + side - dx) % side) * 2 + (c + 2 - dc) % 2
    return to, frm


def moe_kernel(group, side, idx_ref, x_ref, up_ref, down_ref, gate_ref, recv_ref, ret_ref,
               rows, send, blk, gblk, hid, out, send_sem, out_sem, recv_sem, ret_sem, load_sem):
    me = lax.axis_index("ep")
    cap, sub = rows.shape[0], rows.shape[1]

    barrier = pltpu.get_barrier_semaphore()

    def hello(d, _):
        pl.semaphore_signal(barrier, inc=1, device_id={"ep": (me + d) % group}, device_id_type=pl.DeviceIdType.MESH)
        return 0

    lax.fori_loop(1, group, hello, 0)
    pl.semaphore_wait(barrier, group - 1)

    def dispatch(k):
        to, _ = peers(k, group, side)
        return pltpu.make_async_remote_copy(
            src_ref=send.at[k % SEND_SLOTS], dst_ref=recv_ref.at[me], send_sem=send_sem.at[k % SEND_SLOTS],
            recv_sem=recv_sem.at[k], device_id={"ep": to}, device_id_type=pl.DeviceIdType.MESH)

    def give_back(k):
        _, frm = peers(k, group, side)
        return pltpu.make_async_remote_copy(
            src_ref=out.at[k % OUT_SLOTS], dst_ref=ret_ref.at[me], send_sem=out_sem.at[k % OUT_SLOTS],
            recv_sem=ret_sem.at[k], device_id={"ep": frm}, device_id_type=pl.DeviceIdType.MESH)

    def pack(to, dst):
        def pick(b, _):
            vals = [x_ref[idx_ref[to, b * BATCH + j]].astype(jnp.float32) for j in range(BATCH)]
            for j in range(BATCH):
                rows[b * BATCH + j] = vals[j]
            return 0

        lax.fori_loop(0, cap // BATCH, pick, 0)

        def flat(b, _):
            at = pl.ds(b * STEP, STEP)
            for s in range(sub):
                dst[at, s * LANES:(s + 1) * LANES] = rows[at, s, :].astype(jnp.bfloat16)
            return 0

        lax.fori_loop(0, cap // STEP, flat, 0)

    def pack_and_send(k):
        to, _ = peers(k, group, side)

        @pl.when(k > SEND_SLOTS)
        def _():
            dispatch(k - SEND_SLOTS).wait_send()

        pack(to, send.at[k % SEND_SLOTS])
        dispatch(k).start()

    def ffn_up():
        def up(f, _):
            at = pl.ds(pl.multiple_of(f * COLS, COLS), COLS)
            z = jnp.dot(blk[...], up_ref[:, at], preferred_element_type=jnp.float32)
            hid[:, at] = jax.nn.gelu(z, approximate=True).astype(jnp.bfloat16)
            return 0

        lax.fori_loop(0, up_ref.shape[1] // COLS, up, 0)

    def ffn_down(slot):
        for n in range(down_ref.shape[1] // COLS):
            o = jnp.dot(hid[...], down_ref[:, n * COLS:(n + 1) * COLS], preferred_element_type=jnp.float32)
            for t in range(COLS // LANES):
                rows[:, n * (COLS // LANES) + t, :] = o[:, t * LANES:(t + 1) * LANES] * gblk[...]

        def tile(b, _):
            at = pl.ds(b * STEP, STEP)
            out[slot, at] = rows[at].astype(jnp.bfloat16)
            return 0

        lax.fori_loop(0, cap // STEP, tile, 0)

    def own():
        load_gate = pltpu.make_async_copy(gate_ref.at[me], gblk, load_sem.at[1])
        load_gate.start()
        pack(me, blk)
        load_gate.wait()
        ffn_up()
        ffn_down(0)
        keep = pltpu.make_async_copy(out.at[0], ret_ref.at[me], load_sem.at[0])
        keep.start()
        keep.wait()

    def expert(k):
        to, frm = peers(k, group, side)
        pltpu.make_async_remote_copy(
            src_ref=send.at[0], dst_ref=recv_ref.at[frm], send_sem=send_sem.at[0], recv_sem=recv_sem.at[k],
            device_id={"ep": to}, device_id_type=pl.DeviceIdType.MESH).wait_recv()
        load_rows = pltpu.make_async_copy(recv_ref.at[frm], blk, load_sem.at[0])
        load_gate = pltpu.make_async_copy(gate_ref.at[frm], gblk, load_sem.at[1])
        load_rows.start()
        load_gate.start()
        load_rows.wait()
        load_gate.wait()
        ffn_up()

        @pl.when(k > OUT_SLOTS)
        def _():
            give_back(k - OUT_SLOTS).wait_send()

        ffn_down(k % OUT_SLOTS)
        give_back(k).start()

    def first(k, _):
        pack_and_send(k)
        return 0

    def step(k, _):
        @pl.when(k + AHEAD < group)
        def _():
            pack_and_send(k + AHEAD)

        expert(k)
        return 0

    lax.fori_loop(1, min(AHEAD + 1, group), first, 0)
    own()
    lax.fori_loop(1, group, step, 0)

    def drain_send(k, _):
        dispatch(k).wait_send()
        return 0

    def drain_out(k, _):
        give_back(k).wait_send()
        return 0

    def drain_ret(k, _):
        to, _ = peers(k, group, side)
        pltpu.make_async_remote_copy(
            src_ref=out.at[0], dst_ref=ret_ref.at[to], send_sem=out_sem.at[0], recv_sem=ret_sem.at[k],
            device_id={"ep": to}, device_id_type=pl.DeviceIdType.MESH).wait_recv()
        return 0

    lax.fori_loop(max(group - SEND_SLOTS, 1), group, drain_send, 0)
    lax.fori_loop(max(group - OUT_SLOTS, 1), group, drain_out, 0)
    lax.fori_loop(1, group, drain_ret, 0)


def moe_exchange(group, idx, x3, up, down, gates):
    side = math.isqrt(group // 2)
    assert 2 * side * side == group
    cap = idx.shape[1]
    tail = x3.shape[1:]
    width, hidden = up.shape
    any_spec = pl.BlockSpec(memory_space=pl.ANY)
    vmem_spec = pl.BlockSpec(memory_space=pltpu.VMEM)
    _, ret = pl.pallas_call(
        functools.partial(moe_kernel, group, side),
        in_specs=[pl.BlockSpec(memory_space=pltpu.SMEM), vmem_spec, vmem_spec, vmem_spec, any_spec],
        out_specs=[any_spec, any_spec],
        out_shape=[jax.ShapeDtypeStruct((group, cap, width), x3.dtype), jax.ShapeDtypeStruct((group, cap) + tail, x3.dtype)],
        scratch_shapes=[
            pltpu.VMEM((cap,) + tail, jnp.float32),
            pltpu.VMEM((SEND_SLOTS, cap, width), x3.dtype),
            pltpu.VMEM((cap, width), x3.dtype),
            pltpu.VMEM((cap, LANES), jnp.float32),
            pltpu.VMEM((cap, hidden), x3.dtype),
            pltpu.VMEM((OUT_SLOTS, cap) + tail, x3.dtype),
            pltpu.SemaphoreType.DMA((SEND_SLOTS,)),
            pltpu.SemaphoreType.DMA((OUT_SLOTS,)),
            pltpu.SemaphoreType.DMA((group,)),
            pltpu.SemaphoreType.DMA((group,)),
            pltpu.SemaphoreType.DMA((2,)),
        ],
        compiler_params=pltpu.CompilerParams(collective_id=0, has_side_effects=True, vmem_limit_bytes=VMEM_LIMIT),
        cost_estimate=pl.CostEstimate(flops=4 * group * cap * width * hidden, bytes_accessed=4 * group * cap * width, transcendentals=0),
    )(idx, x3, up, down, gates)
    return ret


def combine_kernel(idx_ref, cnt_ref, x_ref, ret_ref, out_ref, acc):
    g = pl.program_id(0)
    part = ret_ref.shape[0]
    tok, width = x_ref.shape
    sub = width // LANES

    @pl.when(g == 0)
    def _():
        def load(b, _):
            at = pl.ds(b * STEP, STEP)
            for s in range(sub):
                acc[at, s, :] = x_ref[at, s * LANES:(s + 1) * LANES].astype(jnp.float32)
            return 0

        lax.fori_loop(0, tok // STEP, load, 0)

    def body(b, _):
        at = [idx_ref[g * part + b * ADD_BATCH + j] for j in range(ADD_BATCH)]
        sums = [acc[at[j]] + ret_ref[b * ADD_BATCH + j].astype(jnp.float32) for j in range(ADD_BATCH)]
        for j in range(ADD_BATCH):
            acc[at[j]] = sums[j]
        return 0

    lax.fori_loop(0, (cnt_ref[g] + ADD_BATCH - 1) // ADD_BATCH, body, 0)

    @pl.when(g == pl.num_programs(0) - 1)
    def _():
        def store(b, _):
            at = pl.ds(b * STEP, STEP)
            for s in range(sub):
                out_ref[at, s * LANES:(s + 1) * LANES] = acc[at, s, :].astype(jnp.bfloat16)
            return 0

        lax.fori_loop(0, tok // STEP, store, 0)


def combine_rows(x_loc, ret, idx, cnt):
    group, part = ret.shape[:2]
    tail = ret.shape[2:]
    tok = x_loc.shape[0]
    whole = pl.BlockSpec(x_loc.shape, lambda g, idx, cnt: (0, 0))
    return pl.pallas_call(
        combine_kernel,
        grid_spec=pltpu.PrefetchScalarGridSpec(
            num_scalar_prefetch=2,
            grid=(group,),
            in_specs=[whole, pl.BlockSpec((None, part) + tail, lambda g, idx, cnt: (g, 0, 0, 0))],
            out_specs=whole,
            scratch_shapes=[pltpu.VMEM((tok + 8,) + tail, jnp.float32)],
        ),
        out_shape=jax.ShapeDtypeStruct(x_loc.shape, x_loc.dtype),
        compiler_params=pltpu.CompilerParams(vmem_limit_bytes=VMEM_LIMIT),
        cost_estimate=pl.CostEstimate(flops=group * part * 4096, bytes_accessed=group * part * 4096, transcendentals=0),
    )(idx, cnt, x_loc, ret)


def solution(mesh):
    group_size = mesh.shape["ep"]

    def local_layer(x_loc, sel_loc, gate_loc, up_loc, down_loc):
        tok_loc, model_width = x_loc.shape
        tail = (model_width // LANES, LANES)
        entry_count = sel_loc.shape[0] * sel_loc.shape[1]
        pair_cap = 2 * entry_count // group_size
        sel = sel_loc.reshape(entry_count)
        dev_ids = jnp.arange(group_size, dtype=jnp.int32)
        src_dev = sel // tok_loc
        counts = jnp.sum((src_dev[:, None] == dev_ids[None, :]).astype(jnp.int32), axis=0)
        lower = dev_ids[:, None] >= dev_ids[None, :]
        free_end = jnp.sum(jnp.where(lower, (pair_cap - counts)[None, :], 0), axis=1)
        fill_ids = jnp.arange(group_size * pair_cap - entry_count, dtype=jnp.int32)
        fill_dev = jnp.sum((free_end[None, :] <= fill_ids[:, None]).astype(jnp.int32), axis=1)
        keys = jnp.concatenate([sel + src_dev * tok_loc, fill_dev * (2 * tok_loc) + tok_loc])
        gates = jnp.concatenate([gate_loc.reshape(entry_count), jnp.zeros(fill_ids.shape, jnp.float32)])
        keys, gates = lax.sort((keys, gates), num_keys=1, is_stable=False)
        request = keys.reshape(group_size, pair_cap) - dev_ids[:, None] * (2 * tok_loc)
        gates = jnp.broadcast_to(gates.reshape(group_size, pair_cap)[:, :, None], (group_size, pair_cap, LANES))
        wanted = lax.all_to_all(request, "ep", 0, 0, tiled=True)
        filled = jnp.sum((wanted < tok_loc).astype(jnp.int32), axis=1)
        x3 = x_loc.reshape((tok_loc,) + tail)
        ret = moe_exchange(group_size, jnp.minimum(wanted, tok_loc - 1), x3, up_loc[0], down_loc[0], gates)
        return combine_rows(x_loc, ret, wanted.reshape(group_size * pair_cap), filled)

    row_spec = P(("dp", "ep"), None)
    weight_spec = P("ep", None, None)
    return jax.shard_map(local_layer, mesh=mesh, in_specs=(row_spec, row_spec, row_spec, weight_spec, weight_spec), out_specs=row_spec, check_vma=False)
```

```python
import functools

import jax
import jax.numpy as jnp
from jax import lax
from jax.experimental import pallas as pl
from jax.experimental.pallas import tpu as pltpu
from jax.sharding import PartitionSpec as P

CHUNKS = 2
LANES = 128
BATCH = 8
ADD_BATCH = 16
STEP = 128
VMEM_LIMIT = 60 * 1024 * 1024


def pack_kernel(idx_ref, x_ref, out_ref):
    rows = out_ref.shape[0]
    base = pl.program_id(0) * rows

    def body(b, _):
        vals = [x_ref[idx_ref[base + b * BATCH + j]] for j in range(BATCH)]
        for j in range(BATCH):
            out_ref[b * BATCH + j] = vals[j]
        return 0

    lax.fori_loop(0, rows // BATCH, body, 0)


def pack_rows(x3, idx, block):
    rows = idx.shape[0]
    tail = x3.shape[1:]
    return pl.pallas_call(
        pack_kernel,
        grid_spec=pltpu.PrefetchScalarGridSpec(
            num_scalar_prefetch=1,
            grid=(rows // block,),
            in_specs=[pl.BlockSpec(x3.shape, lambda i, idx: (0, 0, 0))],
            out_specs=pl.BlockSpec((block,) + tail, lambda i, idx: (i, 0, 0)),
        ),
        out_shape=jax.ShapeDtypeStruct((rows,) + tail, x3.dtype),
        compiler_params=pltpu.CompilerParams(vmem_limit_bytes=VMEM_LIMIT),
        cost_estimate=pl.CostEstimate(flops=rows * 4096, bytes_accessed=rows * 4096, transcendentals=0),
    )(idx, x3)


def combine_kernel(last, idx_ref, cnt_ref, base_ref, ret_ref, out_ref, acc, sem):
    g = pl.program_id(0)
    part = ret_ref.shape[0]
    tok = base_ref.shape[0]

    @pl.when(g == 0)
    def _():
        load = pltpu.make_async_copy(base_ref, acc.at[pl.ds(0, tok)], sem)
        load.start()
        load.wait()

    def body(b, _):
        at = [idx_ref[g * part + b * ADD_BATCH + j] for j in range(ADD_BATCH)]
        sums = [acc[at[j]] + ret_ref[b * ADD_BATCH + j].astype(jnp.float32) for j in range(ADD_BATCH)]
        for j in range(ADD_BATCH):
            acc[at[j]] = sums[j]
        return 0

    lax.fori_loop(0, (cnt_ref[g] + ADD_BATCH - 1) // ADD_BATCH, body, 0)

    @pl.when(g == pl.num_programs(0) - 1)
    def _():
        if last:
            def flat(b, _):
                at = pl.ds(b * STEP, STEP)
                for s in range(acc.shape[1]):
                    out_ref[at, s * LANES:(s + 1) * LANES] = acc[at, s, :].astype(jnp.bfloat16)
                return 0

            lax.fori_loop(0, tok // STEP, flat, 0)
        else:
            store = pltpu.make_async_copy(acc.at[pl.ds(0, tok)], out_ref, sem)
            store.start()
            store.wait()


def combine_rows(base, ret, idx, cnt, last):
    group, part = ret.shape[:2]
    tail = base.shape[1:]
    flat = (base.shape[0], tail[0] * tail[1])
    return pl.pallas_call(
        functools.partial(combine_kernel, last),
        grid_spec=pltpu.PrefetchScalarGridSpec(
            num_scalar_prefetch=2,
            grid=(group,),
            in_specs=[
                pl.BlockSpec(memory_space=pl.ANY),
                pl.BlockSpec((None, part) + tail, lambda g, idx, cnt: (g, 0, 0, 0)),
            ],
            out_specs=pl.BlockSpec(flat, lambda g, idx, cnt: (0, 0)) if last else pl.BlockSpec(memory_space=pl.ANY),
            scratch_shapes=[pltpu.VMEM((base.shape[0] + 8,) + tail, jnp.float32), pltpu.SemaphoreType.DMA],
        ),
        out_shape=jax.ShapeDtypeStruct(flat, jnp.bfloat16) if last else jax.ShapeDtypeStruct(base.shape, jnp.float32),
        compiler_params=pltpu.CompilerParams(vmem_limit_bytes=VMEM_LIMIT),
        cost_estimate=pl.CostEstimate(flops=group * part * 4096, bytes_accessed=group * part * 6144, transcendentals=0),
    )(idx, cnt, base, ret)


def solution(mesh):
    group_size = mesh.shape["ep"]

    def local_layer(x_loc, sel_loc, gate_loc, up_loc, down_loc):
        tok_loc, model_width = x_loc.shape
        tail = (model_width // LANES, LANES)
        entry_count = sel_loc.shape[0] * sel_loc.shape[1]
        pair_cap = 2 * entry_count // group_size
        part = pair_cap // CHUNKS
        sel = sel_loc.reshape(entry_count)
        dev_ids = jnp.arange(group_size, dtype=jnp.int32)
        src_dev = sel // tok_loc
        counts = jnp.sum((src_dev[:, None] == dev_ids[None, :]).astype(jnp.int32), axis=0)
        lower = dev_ids[:, None] >= dev_ids[None, :]
        free_end = jnp.sum(jnp.where(lower, (pair_cap - counts)[None, :], 0), axis=1)
        fill_ids = jnp.arange(group_size * pair_cap - entry_count, dtype=jnp.int32)
        fill_dev = jnp.sum((free_end[None, :] <= fill_ids[:, None]).astype(jnp.int32), axis=1)
        keys = jnp.concatenate([sel + src_dev * tok_loc, fill_dev * (2 * tok_loc) + tok_loc])
        gates = jnp.concatenate([gate_loc.reshape(entry_count), jnp.zeros(fill_ids.shape, jnp.float32)])
        keys, gates = lax.sort((keys, gates), num_keys=1, is_stable=False)
        request = keys.reshape(group_size, pair_cap) - dev_ids[:, None] * (2 * tok_loc)
        gates = gates.reshape(group_size, pair_cap)
        wanted = lax.all_to_all(request, "ep", 0, 0, tiled=True)
        filled = jnp.sum((wanted < tok_loc).astype(jnp.int32), axis=1)

        rows = group_size * part
        x3 = x_loc.reshape((tok_loc,) + tail)
        sent = []
        for k in range(CHUNKS):
            idx = wanted[:, k * part:(k + 1) * part].reshape(rows)
            send = pack_rows(x3, jnp.minimum(idx, tok_loc - 1), rows // 8)
            sent.append((idx, lax.all_to_all(send.reshape((group_size, part) + tail), "ep", 0, 0, tiled=True)))
        back = []
        for k in range(CHUNKS):
            idx, got = sent[k]
            hidden = jax.nn.gelu(jnp.dot(got.reshape(rows, model_width), up_loc[0], preferred_element_type=jnp.float32), approximate=True).astype(jnp.bfloat16)
            out = jnp.dot(hidden, down_loc[0], preferred_element_type=jnp.float32)
            gate = gates[:, k * part:(k + 1) * part].reshape(rows, 1)
            contrib = (out * gate).astype(jnp.bfloat16).reshape((group_size, part) + tail)
            back.append((idx, lax.all_to_all(contrib, "ep", 0, 0, tiled=True)))
        acc = x3.astype(jnp.float32)
        for k, (idx, ret) in enumerate(back):
            acc = combine_rows(acc, ret, idx, jnp.clip(filled - k * part, 0, part), k == CHUNKS - 1)
        return acc

    row_spec = P(("dp", "ep"), None)
    weight_spec = P("ep", None, None)
    return jax.shard_map(local_layer, mesh=mesh, in_specs=(row_spec, row_spec, row_spec, weight_spec, weight_spec), out_specs=row_spec, check_vma=False)
```
